256 devices in a mesh: patch: 32 (over z, y_lo, core), lag: 8 (over x, y_hi).
Axes of the slice: x: 4, y: 4 (y_hi: 2, y_lo: 2; y = y_hi * 2 + y_lo), z: 8, core: 2. Of those that a mesh axis runs over, the one named last changes fastest.
Arguments:
- interaction: bfloat16 [120, 8192, 1280], P('lag', 'patch'), may hold values from -0.0234375 to 0.0234375
- history: bfloat16 [120, 8192, 128], P('lag', 'patch'), may hold values from -6 to 6
- near_inverse: bfloat16 [8192, 256], P('patch'), may hold values from -0.375 to 0.375
- lag_ranges: int32 [32, 10], P('patch'), may hold values from 1 to 121, as said below
- receiver_tile: int32 [8192, 1], P('patch'), may hold values from 0 to 31; in each aligned block of 256 rows (0 to 255, 256 to 511, ...) at most 16 rows name the same one
- receiver_panel: int32 [8192], P('patch'), may hold values from 0 to 255
- residuals: bfloat16 [8192, 4, 128], P('patch'), may hold values from -6 to 6
Outputs:
- densities: bfloat16 [4, 8192, 128], P(None, 'patch')
The draws below stay inside these ranges and needn't reach their ends.
Inputs may be any that keep to these rules, and one draw needn't show every extreme that they name: `lag_ranges`: columns 0 to 4 hold the first active lag, columns 5 to 9 one past the last; every range holds at least 30 lags. `receiver_tile`: among the 256 receivers of one patch index, at most 16 lie on one patch.
All inputs are finite; a program needn't handle non-finite values.
Results may differ from the reference program's by a relative error of at most 0.0049.
Values may be sent and summed in bfloat16 or wider, within the bound.
A program may use at most 64 MiB of HBM per device.

```python
import math
import jax
import jax.numpy as jnp
import numpy as np
from jax import lax

TILE = 256
NEAR = 5
STEPS = 4
SHOTS = 128
RECV_DEV = 256
CAP = 16
TILES = 32
PANELS = 8192
LAGS = 120
RECEIVERS = 8192


def draw_lag_ranges(key, part):
    key_lower, key_count = jax.random.split(jax.random.fold_in(key, 7))
    lower = jax.random.randint(key_lower, (TILES, NEAR), 1, LAGS // 2 + 2)
    counts = jax.random.randint(key_count, (TILES, NEAR), LAGS // 4, LAGS // 2 + 1)
    return jnp.concatenate([lower, lower + counts], 1).astype(jnp.int32)


def plant(array, key, smallest, high):
    shape = array.shape
    index_at = [jax.random.randint(jax.random.fold_in(key, axis), (), 0, shape[axis]) for axis in range(len(shape))]
    array = array.at[tuple(index_at)].set(smallest)
    longest = shape.index(max(shape))
    index_at[longest] = (index_at[longest] + 1) % shape[longest]
    return array.at[tuple(index_at)].set(high)


def shard_levels(key, extent, cuts, least, top_value):
    level, own = 1.0, jax.random.fold_in(key, 6)
    for axis_at, shards_of in cuts:
        heights = jnp.exp(jax.random.uniform(jax.random.fold_in(own, axis_at), (shards_of,), jnp.float32, least / len(cuts), top_value / len(cuts)))
        level = level * jnp.repeat(heights, extent[axis_at] // shards_of).reshape([-1 if axis == axis_at else 1 for axis in range(len(extent))])
    return level


def assign_block(key, own, number, rows, amount, top, bound, lean):
    sequence = jax.random.permutation(key, amount)
    crowded, usual = shares(amount, rows * top, bound, lean, True), shares(amount, rows * top, bound, lean, False)
    places = jnp.arange(amount)

    def named(sizes, turn):
        used = int((sizes > 0).sum())
        fixed = max(1, used // 4)
        moved = fixed + (places - fixed + turn * (used - fixed)) % max(1, amount - fixed)
        return jnp.zeros((amount,), jnp.int32).at[sequence[jnp.where(places < fixed, places, moved)]].set(jnp.asarray(sizes, jnp.int32))

    sizes = jnp.where(number % 4 == 0, named(crowded, number // 4), named(usual, number - number // 4 - 1))
    mixed = jax.random.permutation(jax.random.fold_in(own, 3), amount)
    giver, taker = mixed[0:amount // 2 * 2:2], mixed[1:amount // 2 * 2:2]
    margin = jnp.minimum(sizes[giver] - 1, bound - sizes[taker]) // 2
    margin = jnp.where((giver == sequence[0]) | (taker == sequence[0]) | (sizes[taker] == 0), 0, jnp.maximum(margin, 0))
    moved = jax.random.randint(jax.random.fold_in(own, 4), (amount // 2,), 0, 1 << 20) % (margin + 1)
    sizes = sizes.at[giver].add(-moved).at[taker].add(moved)
    labels = jnp.searchsorted(jnp.cumsum(sizes), jnp.arange(rows * top), side="right").astype(jnp.int32)
    table = labels.reshape(top, rows).T
    table = table[jax.random.permutation(jax.random.fold_in(own, 1), rows)]
    turn = jax.random.randint(jax.random.fold_in(own, 2), (rows, 1), 0, top)
    return jnp.take_along_axis(table, (jnp.arange(top)[None, :] + turn) % top, axis=1)


def shares(count, total, limit, slope, full):
    portions = [(1 << 20) // math.isqrt(grade ** slope) + 1 for grade in range(1, count + 1)]
    largest = limit if full else min(limit, max(-(-total // count), total * portions[0] // sum(portions)))
    least = 1 if total - largest >= count - 1 else 0
    given, rest = [largest] + [least] * (count - 1), total - largest - least * (count - 1)
    while rest > 0:
        movable = [i for i in range(1, count) if given[i] < largest] or [i for i in range(1, count) if given[i] < limit]
        mass, budget = sum([portions[i] for i in movable]), rest
        for i in movable:
            addition = min(limit - given[i], max(1, budget * portions[i] // mass), rest)
            given[i] = given[i] + addition
            rest = rest - addition
    return np.array(given)


def normal_values(rng, extent, deviation, bound, pieces=(), kind=jnp.bfloat16):
    array = jax.random.normal(rng, extent, jnp.float32) * deviation
    if len(pieces) > 0:
        array = shard_levels(rng, extent, pieces, -0.22, 0.18) * array
    return jnp.clip(array, min=-bound, max=bound).astype(kind)


def setup_inputs(seed: int = 0) -> dict:
    key_of = jax.random.split(jax.random.key(seed), 8)
    interaction = normal_values(key_of[0], (LAGS, PANELS, NEAR * TILE), (3 * LAGS * NEAR * TILE // 8) ** -0.5, 0.0234375, ((0, 8), (1, 32)))
    history = normal_values(key_of[1], (LAGS, PANELS, SHOTS), 1.0, 6.0, ((0, 8), (1, 32)))
    near_inverse = normal_values(key_of[2], (PANELS, TILE), TILE ** -0.5, 0.375, ((0, 32),))
    lag_ranges = draw_lag_ranges(jax.random.fold_in(key_of[7], 71), 0)
    receiver_tile_keys = jax.random.split(jax.random.fold_in(key_of[4], 1), RECEIVERS // RECV_DEV)
    receiver_tile_turns = jax.random.permutation(jax.random.fold_in(key_of[4], 3), RECEIVERS // RECV_DEV)
    receiver_tile = jax.vmap(lambda own, number: assign_block(jax.random.fold_in(key_of[4], 2), own, number, RECV_DEV, TILES, 1, CAP, 2))(receiver_tile_keys, receiver_tile_turns).reshape((RECEIVERS, 1))
    receiver_panel = plant(jax.random.randint(key_of[5], (RECEIVERS,), 0, TILE), jax.random.fold_in(key_of[5], 1), 0, TILE - 1).astype(jnp.int32)
    residuals = normal_values(key_of[6], (RECEIVERS, STEPS, SHOTS), 1.0, 6.0, ((0, 32),))
    return {"interaction": interaction, "history": history, "near_inverse": near_inverse, "lag_ranges": lag_ranges, "receiver_tile": receiver_tile, "receiver_panel": receiver_panel, "residuals": residuals}


def reference(interaction, history, near_inverse, lag_ranges, receiver_tile, receiver_panel, residuals):
    half_near = NEAR // 2
    target = (receiver_tile[:, 0] * TILE + receiver_panel).astype(jnp.int32)
    source = jax.ops.segment_sum(residuals.astype(jnp.float32), target, num_segments=PANELS)
    lag_numbers = jnp.arange(1, LAGS + 1, dtype=jnp.int32)
    lower = lag_ranges[:, :NEAR]
    upper = lag_ranges[:, NEAR:]
    active = ((lag_numbers[:, None, None] >= lower[None]) & (lag_numbers[:, None, None] < upper[None])).astype(jnp.float32)
    blocks = interaction.reshape(LAGS, TILES, TILE, NEAR, TILE)
    inverse = near_inverse.reshape(TILES, TILE, TILE).astype(jnp.float32)
    results = []
    for step_idx in range(STEPS):
        older = history[:LAGS - step_idx]
        if step_idx > 0:
            window = jnp.concatenate([jnp.stack(results[::-1]), older], 0)
        else:
            window = older

        def add_lag(totals, inputs):
            lag_block, lag_rows, lag_mask = inputs
            terms = jnp.einsum("prot,prs->pots", lag_block.astype(jnp.float32),
                               lag_rows.reshape(TILES, TILE, SHOTS).astype(jnp.float32))
            return totals + terms * lag_mask[:, :, None, None], None

        zeros_init = jnp.zeros((TILES, NEAR, TILE, SHOTS), jnp.float32)
        totals, _ = lax.scan(add_lag, zeros_init, (blocks, window, active))
        incoming = jnp.zeros((TILES, TILE, SHOTS), jnp.float32)
        for offset in range(NEAR):
            incoming = incoming + jnp.roll(totals[:, offset], offset - half_near, axis=0)
        right = (source[:, step_idx].reshape(TILES, TILE, SHOTS) - incoming).astype(jnp.bfloat16)
        density = jnp.einsum("prc,prs->pcs", inverse, right.astype(jnp.float32))
        results.append(density.astype(jnp.bfloat16).reshape(PANELS, SHOTS))
    return jnp.stack(results)
```

```python
import functools

import jax
import jax.numpy as jnp
from jax import lax
from jax.experimental import pallas as pl
from jax.experimental.pallas import tpu as pltpu
from jax.sharding import PartitionSpec as P

NEAR = 5
HALF = NEAR // 2
CAP = 16
MESH = pl.DeviceIdType.MESH
F32 = jnp.float32
BF16 = jnp.bfloat16


def remote(src, dst, send, recv, patch, lag):
    return pltpu.make_async_remote_copy(
        src_ref=src,
        dst_ref=dst,
        send_sem=send,
        recv_sem=recv,
        device_id={"patch": patch, "lag": lag},
        device_id_type=MESH,
    )


def dot(a, b):
    return jnp.dot(a, b, preferred_element_type=F32)


def dot_rows(a, b):
    return lax.dot_general(a, b, (((0,), (0,)), ((), ())), preferred_element_type=F32)


def iota(shape, dim):
    return lax.broadcasted_iota(jnp.int32, shape, dim)


def kernel(
    patches, lags, w_hbm, h_hbm, inv_ref, range_ref, tile_ref, panel_ref, resid_ref, out_ref,
    w_buf, h_buf, rim_buf, ht, acc, sbuf, rbuf, nsend, nbuf, src_out, src_in, source, dens, cacc, csend, cbuf,
    w_sem, h_sem, rim_ss, rim_rs, src_ss, src_rs, rs_ss, rs_rs, nb_ss, nb_rs, ag_ss, ag_rs, ch_ss, ch_rs,
):
    t, l = lax.axis_index("patch"), lax.axis_index("lag")
    band, width, cols = w_buf.shape
    steps, shots, _ = sbuf.shape
    chunk = shots // lags
    rim = steps - 1
    is_first = l == 0

    def patch_at(d):
        return lax.rem(t + d + patches, patches)

    def lag_at(d):
        return lax.rem(l + d, lags)

    h_copy = pltpu.make_async_copy(h_hbm, h_buf, h_sem)
    h_copy.start()

    def w_copy(j):
        return pltpu.make_async_copy(w_hbm.at[j], w_buf.at[j], w_sem.at[j])

    for j in [*range(rim, band), *range(rim)]:
        w_copy(j).start()

    barrier = pltpu.get_barrier_semaphore()

    def greet(patch, lag):
        pl.semaphore_signal(barrier, inc=1, device_id={"patch": patch, "lag": lag}, device_id_type=MESH)

    for d in range(1, lags):
        greet(t, lag_at(d))

    def greet_patch(d, carry):
        greet(patch_at(d), l)
        return carry

    lax.fori_loop(1, patches, greet_patch, 0)
    near_by = [d for d in range(-HALF, HALF + 1) if d != 0]

    @pl.when(is_first)
    def _():
        for d in near_by:
            for other in range(1, lags):
                greet(patch_at(d), other)

    @pl.when(l != 0)
    def _():
        for d in near_by:
            greet(patch_at(d), 0)

    recv = tile_ref.shape[1]
    diagonal = iota((recv, recv), 0) == iota((recv, recv), 1)

    def as_column(row):
        return jnp.sum(jnp.where(diagonal, row.astype(F32), 0.0), axis=1, keepdims=True)

    tile_col = as_column(tile_ref[...])
    panel_col = as_column(panel_ref[...])
    named = (tile_col == iota((recv, 128), 1).astype(F32)).astype(F32)
    earlier = (iota((recv, recv), 1) < iota((recv, recv), 0)).astype(BF16)
    rank = jnp.sum(dot(earlier, named.astype(BF16)) * named, axis=1, keepdims=True)
    slot = tile_col * CAP + rank
    placer = (slot == iota((recv, patches * CAP), 1).astype(F32)).astype(BF16)
    src_width = src_out.shape[1]
    mine = jnp.zeros((recv, src_width), F32)
    for s in range(steps):
        lane, place = iota((shots, src_width), 0), iota((shots, src_width), 1)
        pick = (lane - l * chunk == place - s * chunk) & (place >= s * chunk) & (place < (s + 1) * chunk)
        mine = mine + dot(resid_ref[s], pick.astype(BF16))
    mine = jnp.where(iota((recv, src_width), 1) == steps * chunk, panel_col + 1.0, mine).astype(BF16)
    src_out[...] = dot_rows(placer, mine).astype(BF16)
    own_slots = pl.ds(pl.multiple_of(t * CAP, CAP), CAP)
    src_in[own_slots, :] = src_out[own_slots, :]

    h_copy.wait()
    pl.semaphore_wait(barrier, jnp.where(is_first, lags - 1 + patches - 1 + 4 * (lags - 1), lags - 1 + patches - 1 + 4))

    rim_copy = remote(h_buf.at[pl.ds(band - rim, rim)], rim_buf, rim_ss, rim_rs, t, lag_at(1))
    rim_copy.start()

    def slots(p):
        return pl.ds(pl.multiple_of(p * CAP, CAP), CAP)

    def src_copy(d):
        to = patch_at(d)
        return remote(src_out.at[slots(to)], src_in.at[own_slots], src_ss.at[to], src_rs.at[t], to, l)

    def src_start(d, carry):
        src_copy(d).start()
        return carry

    lax.fori_loop(1, patches, src_start, 0)

    def turn(j, carry):
        ht[pl.ds(pl.multiple_of((band - 1 - j) * shots, shots), shots), :] = h_buf[j].T
        return carry

    lax.fori_loop(0, band, turn, 0)
    acc[...] = jnp.zeros_like(acc)

    def is_active(lag_number, i):
        low, high = range_ref[0, i], range_ref[0, NEAR + i]
        return jnp.where((lag_number >= low) & (lag_number < high), 1.0, 0.0).astype(F32)

    def add_lag(j, first_row, rows):
        for i in range(NEAR):
            at = pl.ds(i * width, width)
            left = ht[pl.ds(pl.multiple_of((band - 1 - j) * shots + first_row, shots), rows), :]
            acc[pl.ds(first_row, rows), at] += is_active(l * band + j + 1, i) * dot(left, w_buf[j, :, at])

    def later_lag(j, carry):
        w_copy(j).wait()
        add_lag(j, 0, steps * shots)
        return carry

    def early_lag(j, carry):
        w_copy(j).wait()
        add_lag(j, 0, shots)
        return carry

    def early_lag_rest(j, carry):
        add_lag(j, shots, (steps - 1) * shots)
        return carry

    lax.fori_loop(rim, band, later_lag, 0)
    lax.fori_loop(0, rim, early_lag, 0)

    def rs_copy(s, d):
        to = lag_at(d)
        part = pl.ds(pl.multiple_of(to * chunk, chunk), chunk)
        return remote(sbuf.at[s, part], rbuf.at[s, l], rs_ss.at[s, to], rs_rs.at[s, l], t, to)

    def send_step(s):
        sbuf[s] = acc[pl.ds(s * shots, shots), :].astype(BF16)
        for d in range(1, lags):
            rs_copy(s, d).start()

    send_step(0)
    rim_copy.wait()
    for q in range(rim):
        before = rim_buf[q]
        ht[pl.ds((band + rim - 1 - q) * shots, shots), :] = jnp.where(is_first, jnp.zeros_like(before.T), before.T)
    lax.fori_loop(0, rim, early_lag_rest, 0)
    for s in range(1, steps):
        send_step(s)

    def src_wait(d, carry):
        of = patch_at(d)
        remote(src_in.at[slots(of)], src_in.at[slots(of)], src_ss.at[of], src_rs.at[of], of, l).wait_recv()
        return carry

    lax.fori_loop(1, patches, src_wait, 0)
    labels = src_in[:, pl.ds(steps * chunk, 1)].astype(F32)
    onto = (labels == (iota((patches * CAP, width), 1) + 1).astype(F32)).astype(BF16)
    source[...] = dot_rows(src_in[...], onto)

    own_shots = pl.ds(pl.multiple_of(l * chunk, chunk), chunk)

    def nb_copy(s, i):
        return remote(nsend.at[s, i], nbuf.at[s, i], nb_ss.at[s, i], nb_rs.at[s, i], patch_at(i - HALF), l)

    def ag_copy(s, d):
        to = lag_at(d)
        return remote(dens.at[s, own_shots], dens.at[s, own_shots], ag_ss.at[s, to], ag_rs.at[s, l], t, to)

    def ag_wait(s):
        for d in range(1, lags):
            of = lag_at(d)
            part = pl.ds(pl.multiple_of(of * chunk, chunk), chunk)
            remote(dens.at[s, part], dens.at[s, part], ag_ss.at[s, of], ag_rs.at[s, of], t, of).wait_recv()

    def ch_copy(n, i, lag):
        return remote(
            csend.at[n - 1, pl.ds(lag * chunk, chunk), pl.ds(i * width, width)],
            cbuf.at[n - 1, i], ch_ss.at[n - 1, i * lags + lag], ch_rs.at[n - 1, i], patch_at(i - HALF), lag,
        )

    def new_terms(k, s, i):
        return is_active(k, i) * dot(dens[s], w_buf[k - 1, :, pl.ds(i * width, width)])

    for s in range(steps):
        if s > 0:
            @pl.when(is_first)
            def _():
                ag_wait(s - 1)
                for i in range(NEAR):
                    at = pl.ds(i * width, width)
                    value = new_terms(1, s - 1, i)
                    if s > 1:
                        value = value + cacc[s - 2, :, at]
                    csend[s - 1, :, at] = value.astype(BF16)
                    for lag in range(lags):
                        if i == HALF and lag == 0:
                            cbuf[s - 1, i] = value[:chunk].astype(BF16)
                        else:
                            ch_copy(s, i, lag).start()

        total = acc[pl.ds(pl.multiple_of(s * shots + l * chunk, chunk), chunk), :]
        for d in range(1, lags):
            of = lag_at(d)
            remote(rbuf.at[s, of], rbuf.at[s, of], rs_ss.at[s, of], rs_rs.at[s, of], t, of).wait_recv()
            total = total + rbuf[s, of].astype(F32)
        for i in range(NEAR):
            if i == HALF:
                nbuf[s, i] = total[:, i * width : (i + 1) * width]
            else:
                nsend[s, i] = total[:, i * width : (i + 1) * width]
                nb_copy(s, i).start()
        if 0 < s < steps - 1:
            @pl.when(is_first)
            def _():
                for n in range(s + 1, steps):
                    k = n - s + 1
                    for i in range(NEAR):
                        at = pl.ds(i * width, width)
                        value = new_terms(k, s - 1, i)
                        if s > 1:
                            value = value + cacc[n - 2, :, at]
                        cacc[n - 2, :, at] = value
        incoming = nbuf[s, HALF]
        for i in range(NEAR):
            if i != HALF:
                remote(nbuf.at[s, i], nbuf.at[s, i], nb_ss.at[s, i], nb_rs.at[s, i], patch_at(HALF - i), l).wait_recv()
                incoming = incoming + nbuf[s, i]
        if s > 0:
            for i in range(NEAR):
                arrival = remote(cbuf.at[s - 1, i], cbuf.at[s - 1, i], ch_ss.at[s - 1, 0], ch_rs.at[s - 1, i], patch_at(HALF - i), 0)
                if i != HALF:
                    arrival.wait_recv()
                else:
                    pl.when(l != 0)(arrival.wait_recv)
                incoming = incoming + cbuf[s - 1, i].astype(F32)
        right = (source[pl.ds(s * chunk, chunk), :] - incoming).astype(BF16)
        dens[s, own_shots, :] = dot(right, inv_ref[...]).astype(BF16)
        for d in range(1, lags):
            ag_copy(s, d).start()

    for s in range(steps):
        if s < steps - 1:
            @pl.when(l != 0)
            def _():
                ag_wait(s)
        else:
            ag_wait(s)
    out_ref[...] = dens[...]

    def src_sent(d, carry):
        src_copy(d).wait_send()
        return carry

    lax.fori_loop(1, patches, src_sent, 0)
    for s in range(steps):
        for d in range(1, lags):
            rs_copy(s, d).wait_send()
            ag_copy(s, d).wait_send()
        for i in range(NEAR):
            if i != HALF:
                nb_copy(s, i).wait_send()

    @pl.when(is_first)
    def _():
        for n in range(1, steps):
            for i in range(NEAR):
                for lag in range(lags):
                    if not (i == HALF and lag == 0):
                        ch_copy(n, i, lag).wait_send()


def local(patches, lags, interaction, history, near_inverse, lag_ranges, receiver_tile, receiver_panel, residuals):
    band, width, cols = interaction.shape
    shots = history.shape[2]
    recv, steps, _ = residuals.shape
    chunk = shots // lags
    src_width = -(-(steps * chunk + 1) // 128) * 128
    any_space = pl.BlockSpec(memory_space=pl.ANY)
    vmem = pl.BlockSpec(memory_space=pltpu.VMEM)
    dma = pltpu.SemaphoreType.DMA
    out = pl.pallas_call(
        functools.partial(kernel, patches, lags),
        out_shape=jax.ShapeDtypeStruct((steps, shots, width), BF16),
        in_specs=[any_space, any_space, vmem, pl.BlockSpec(memory_space=pltpu.SMEM), vmem, vmem, vmem],
        out_specs=vmem,
        scratch_shapes=[
            pltpu.VMEM((band, width, cols), BF16),
            pltpu.VMEM((band, width, shots), BF16),
            pltpu.VMEM((steps - 1, width, shots), BF16),
            pltpu.VMEM(((band + steps - 1) * shots, width), BF16),
            pltpu.VMEM((steps * shots, cols), F32),
            pltpu.VMEM((steps, shots, cols), BF16),
            pltpu.VMEM((steps, lags, chunk, cols), BF16),
            pltpu.VMEM((steps, NEAR, chunk, width), F32),
            pltpu.VMEM((steps, NEAR, chunk, width), F32),
            pltpu.VMEM((patches * CAP, src_width), BF16),
            pltpu.VMEM((patches * CAP, src_width), BF16),
            pltpu.VMEM((src_width, width), F32),
            pltpu.VMEM((steps, shots, width), BF16),
            pltpu.VMEM((steps - 2, shots, cols), F32),
            pltpu.VMEM((steps - 1, shots, cols), BF16),
            pltpu.VMEM((steps - 1, NEAR, chunk, width), BF16),
            dma((band,)), dma, dma, dma, dma((patches,)), dma((patches,)),
            dma((steps, lags)), dma((steps, lags)), dma((steps, NEAR)), dma((steps, NEAR)),
            dma((steps, lags)), dma((steps, lags)), dma((steps - 1, NEAR * lags)), dma((steps - 1, NEAR)),
        ],
        compiler_params=pltpu.CompilerParams(collective_id=0, has_side_effects=True, vmem_limit_bytes=60 * 1024 * 1024),
        name="march",
    )(
        interaction, history, near_inverse, lag_ranges, receiver_tile.reshape(1, recv), receiver_panel.reshape(1, recv),
        jnp.swapaxes(residuals, 0, 1),
    )
    return jnp.swapaxes(out, 1, 2)


def solution(mesh):
    in_specs = (
        P("lag", "patch", None),
        P("lag", "patch", None),
        P("patch", None),
        P("patch", None),
        P("patch", None),
        P("patch"),
        P("patch", None, None),
    )
    body = functools.partial(local, mesh.shape["patch"], mesh.shape["lag"])
    return jax.shard_map(body, mesh=mesh, in_specs=in_specs, out_specs=P(None, "patch", None), check_vma=False)
```

```python
import functools

import jax
import jax.numpy as jnp
from jax import lax
from jax.experimental import pallas as pl
from jax.experimental.pallas import tpu as pltpu
from jax.sharding import PartitionSpec as P

NEAR = 5
HALF = NEAR // 2
CAP = 16
GROUPS = 2
MESH = pl.DeviceIdType.MESH
F32 = jnp.float32
BF16 = jnp.bfloat16


def remote(src, dst, send, recv, patch, lag):
    return pltpu.make_async_remote_copy(
        src_ref=src,
        dst_ref=dst,
        send_sem=send,
        recv_sem=recv,
        device_id={"patch": patch, "lag": lag},
        device_id_type=MESH,
    )


def landed(region, sem):
    pltpu.make_async_copy(region, region, sem).wait()


def dot(a, b):
    return jnp.dot(a, b, preferred_element_type=F32)


def dot_rows(a, b):
    return lax.dot_general(a, b, (((0,), (0,)), ((), ())), preferred_element_type=F32)


def iota(shape, dim):
    return lax.broadcasted_iota(jnp.int32, shape, dim)


def kernel(
    patches, lags, w_hbm, h_hbm, inv_hbm, range_ref, tile_ref, panel_ref, resid_hbm, out_ref,
    w_buf, h_buf, inv_ref, resid_ref, rim_buf, ht, acc, got, sbuf, rbuf, psend, own_send, pbuf, nsend, nbuf, own_last, src_out, src_in, source, dens, cacc, csend, cgot, cbuf,
    w_sem, h_sem, inv_sem, resid_sem, rim_ss, rim_rs, src_ss, src_rs, rs_ss, rs_rs, p_ss, p_rs, nb_ss, nb_rs,
    ag_ss, ag_rs, pass_ss, pair_ss, pair_rs, ch_ss, ch_rs, out_ss, out_rs, sp_ss, sp_rs,
):
    t, l = lax.axis_index("patch"), lax.axis_index("lag")
    band, width, cols = w_buf.shape
    core = lax.rem(t, 2)
    given, kept = HALF * width, (HALF + 1) * width
    steps, shots, _ = sbuf.shape
    chunk = shots // lags
    rim = steps - 1
    groups = GROUPS
    group = shots // groups
    is_first = l == 0

    def patch_at(d):
        return lax.rem(t + d + patches, patches)

    def lag_at(d):
        return lax.rem(l + d, lags)

    resid_copy = pltpu.make_async_copy(resid_hbm, resid_ref, resid_sem)
    resid_copy.start()
    h_copy = pltpu.make_async_copy(h_hbm, h_buf, h_sem)
    h_copy.start()
    inv_copy = pltpu.make_async_copy(inv_hbm, inv_ref, inv_sem)

    per = band // w_sem.shape[0]

    def w_copy(a):
        lags_of = pl.ds(a * per, per)
        return pltpu.make_async_copy(w_hbm.at[lags_of], w_buf.at[lags_of], w_sem.at[a])

    w_copy(0).start()

    barrier = pltpu.get_barrier_semaphore()

    def greet(patch, lag):
        pl.semaphore_signal(barrier, inc=1, device_id={"patch": patch, "lag": lag}, device_id_type=MESH)

    for d in range(1, lags):
        greet(t, lag_at(d))

    def greet_patch(d, carry):
        greet(patch_at(d), l)
        return carry

    lax.fori_loop(1, patches, greet_patch, 0)
    near_by = [d for d in range(-HALF, HALF + 1) if d != 0]

    @pl.when(is_first)
    def _():
        for d in near_by:
            for other in range(1, lags):
                greet(patch_at(d), other)

    @pl.when(l != 0)
    def _():
        for d in near_by:
            greet(patch_at(d), 0)

    def turn(j, carry):
        ht[pl.ds(pl.multiple_of((band - 1 - j) * shots, shots), shots), :] = h_buf[j].T
        return carry

    with jax.named_scope("turn"):
        h_copy.wait()
        for a in range(1, band // per):
            w_copy(a).start()
        inv_copy.start()
        lax.fori_loop(0, band, turn, 0)

    def is_active(lag_number, i):
        low, high = range_ref[0, i], range_ref[0, NEAR + i]
        return jnp.where((lag_number >= low) & (lag_number < high), 1.0, 0.0).astype(F32)

    def patch_block(q):
        return q + (HALF + 1) * (1 - core) if q < HALF else q - HALF + HALF * core

    def lag_terms(j, q, first_row, rows):
        i = patch_block(q)
        left = ht[pl.ds(pl.multiple_of((band - 1 - j) * shots + first_row, shots), rows), :]
        right = w_buf[j, :, pl.ds(pl.multiple_of(i * width, width), width)]
        return is_active(l * band + j + 1, i) * dot(left, right)

    def add_lag(j, first_row, rows):
        for q in range(NEAR):
            acc[pl.ds(first_row, rows), pl.ds(q * width, width)] += lag_terms(j, q, first_row, rows)

    def set_lag(j, first_row, rows):
        for q in range(NEAR):
            acc[pl.ds(first_row, rows), pl.ds(q * width, width)] = lag_terms(j, q, first_row, rows)

    def pair_copy(first, count, at):
        rows = pl.ds(first * shots, count * shots)
        return remote(acc.at[rows, pl.ds(0, given)], got.at[rows], pair_ss, pair_rs.at[at], t + 1 - 2 * core, l)

    def pair_wait(first, count):
        landed(got.at[pl.ds(first * shots, count * shots)], pair_rs.at[min(first, 2)])

    def first_step(j, carry):
        add_lag(j, 0, shots)
        return carry

    def later_steps(j, carry):
        add_lag(j, shots, (steps - 1) * shots)
        return carry

    def second_step_rim(j, carry):
        add_lag(j, shots, shots)
        return carry

    def last_steps_rim(j, carry):
        add_lag(j, 2 * shots, (steps - 2) * shots)
        return carry

    def rim_copy(first, count, at):
        return remote(h_buf.at[pl.ds(band - rim + first, count)], rim_buf.at[pl.ds(first, count)], rim_ss.at[at], rim_rs.at[at], t, lag_at(1))

    def turn_rim(q):
        before = rim_buf[q].T
        ht[pl.ds((band + rim - 1 - q) * shots, shots), :] = jnp.where(is_first, jnp.zeros_like(before), before)

    def slots(p):
        return pl.ds(pl.multiple_of(p * CAP, CAP), CAP)

    own_slots = pl.ds(pl.multiple_of(t * CAP, CAP), CAP)

    def src_copy(d):
        to = patch_at(d)
        return remote(src_out.at[slots(to)], src_in.at[own_slots], src_ss, src_rs, to, l)

    def src_start(d, carry):
        src_copy(d).start()
        return carry

    def rs_copy(s, d):
        to = lag_at(d)
        part = pl.ds(pl.multiple_of(to * chunk, chunk), chunk)
        return remote(sbuf.at[s, part], rbuf.at[s, l], rs_ss, rs_rs.at[s], t, to)

    def send_step(s):
        rows = pl.ds(s * shots, shots)
        shared = pl.ds(pl.multiple_of(given + width * (1 - core), width), given)
        acc[rows, shared] += got[rows, :]
        sbuf[s] = acc[rows, pl.ds(given, kept)].astype(BF16)
        for d in range(1, lags):
            rs_copy(s, d).start()

    own_shots = pl.ds(pl.multiple_of(l * chunk, chunk), chunk)

    last = steps - 1

    def lag_sum(s):
        total = acc[pl.ds(pl.multiple_of(s * shots + l * chunk, chunk), chunk), pl.ds(given, kept)]
        landed(rbuf.at[s, pl.ds(0, lags - 1)], rs_rs.at[s])
        for d in range(1, lags):
            total = total + rbuf[s, lag_at(d)].astype(F32)
        parts = [total[:, m * width : (m + 1) * width] for m in range(HALF + 1)]
        own = jnp.where(core == 0, parts[HALF], parts[0]) - source[pl.ds(s * chunk, chunk), :]
        return parts, own

    def owner(f):
        return patch_at(f - HALF + (HALF + 1) * core)

    def piece_rows(side, lag):
        return pl.ds(pl.multiple_of(side * shots + lag * chunk, chunk), chunk)

    def piece_copy(s, f):
        return remote(psend.at[s, f + core], pbuf.at[s, piece_rows(HALF - core, l)], p_ss, p_rs.at[s], owner(f), 0)

    def own_piece_copy(s):
        return remote(own_send.at[s], pbuf.at[s, piece_rows(0, l)], p_ss, p_rs.at[s], t, 0)

    def pieces(s):
        parts, own = lag_sum(s)
        for m in range(HALF + 1):
            psend[s, m] = parts[m].astype(BF16)
        for f in range(HALF):
            piece_copy(s, f).start()

        @pl.when(is_first)
        def _():
            pbuf[s, pl.ds(0, chunk), :] = own.astype(BF16)

        @pl.when(l != 0)
        def _():
            own_send[s] = own.astype(BF16)
            own_piece_copy(s).start()

    def piece_wait(s):
        landed(pbuf.at[s, pl.ds(chunk, (HALF + 1) * shots - chunk)], p_rs.at[s])

    def piece_sum(s, first, count):
        sides = [pbuf[s, pl.ds(side * shots + first, count), :].astype(F32) for side in range(HALF + 1)]
        return sides[0] + sides[1] + sides[2]

    def nb_copy(f):
        return remote(nsend.at[f + core], nbuf.at[1 - core], nb_ss, nb_rs, owner(f), l)

    def last_sum():
        parts, own = lag_sum(last)
        for m in range(HALF + 1):
            nsend[m] = parts[m]
        for f in range(HALF):
            nb_copy(f).start()
        return own

    def nb_sum(own):
        landed(nbuf, nb_rs)
        return own + nbuf[0] + nbuf[1]

    def density_of(right):
        return dot(right.astype(BF16), inv_ref[...]).astype(BF16)

    def ag_copy(s, d, sent):
        return remote(dens.at[s, own_shots], dens.at[s, own_shots], sent, ag_rs, t, lag_at(d))

    with jax.named_scope("first"):
        w_copy(0).wait()
        set_lag(0, 0, shots)
        lax.fori_loop(1, per, first_step, 0)
        for a in range(1, band // per):
            w_copy(a).wait()
            lax.fori_loop(a * per, (a + 1) * per, first_step, 0)
    with jax.named_scope("bar"):
        pl.semaphore_wait(barrier, jnp.where(is_first, lags - 1 + patches - 1 + 4 * (lags - 1), lags - 1 + patches - 1 + 4))
    with jax.named_scope("pair0"):
        pair_copy(0, 1, 0).start()
        rim_copy(rim - 1, 1, 0).start()

    with jax.named_scope("prep"):
        recv = tile_ref.shape[1]
        diagonal = iota((recv, recv), 0) == iota((recv, recv), 1)

        def as_column(row):
            return jnp.sum(jnp.where(diagonal, row.astype(F32), 0.0), axis=1, keepdims=True)

        tile_col = as_column(tile_ref[...])
        panel_col = as_column(panel_ref[...])
        named = (tile_col == iota((recv, 128), 1).astype(F32)).astype(F32)
        earlier = (iota((recv, recv), 1) < iota((recv, recv), 0)).astype(BF16)
        rank = jnp.sum(dot(earlier, named.astype(BF16)) * named, axis=1, keepdims=True)
        slot = tile_col * CAP + rank
        placer = (slot == iota((recv, patches * CAP), 1).astype(F32)).astype(BF16)
        src_width = src_out.shape[1]
        mine = jnp.zeros((recv, src_width), F32)
        resid_copy.wait()
        for s in range(steps):
            lane, place = iota((shots, src_width), 0), iota((shots, src_width), 1)
            pick = (lane - l * chunk == place - s * chunk) & (place >= s * chunk) & (place < (s + 1) * chunk)
            mine = mine + dot(resid_ref[:, s, :], pick.astype(BF16))
        mine = jnp.where(iota((recv, src_width), 1) == steps * chunk, panel_col + 1.0, mine).astype(BF16)
        src_out[...] = dot_rows(placer, mine).astype(BF16)
        src_in[own_slots, :] = src_out[own_slots, :]

    with jax.named_scope("src0"):
        lax.fori_loop(1, patches, src_start, 0)
    with jax.named_scope("pairwait0"):
        pair_wait(0, 1)
    with jax.named_scope("send0"):
        send_step(0)
        rim_copy(0, rim - 1, 1).start()
    with jax.named_scope("later2"):
        set_lag(rim, shots, (steps - 1) * shots)
        lax.fori_loop(rim + 1, band, later_steps, 0)

    with jax.named_scope("rim1"):
        rim_copy(rim - 1, 1, 0).wait()
        turn_rim(rim - 1)
        lax.fori_loop(0, rim, second_step_rim, 0)
        pair_copy(1, 1, 1).start()

    with jax.named_scope("srcwait"):
        landed(src_in.at[pl.ds(0, (patches - 1) * CAP)], src_rs)
        inv_copy.wait()
    with jax.named_scope("src"):
        labels = src_in[:, pl.ds(steps * chunk, 1)].astype(F32)
        onto = (labels == (iota((patches * CAP, width), 1) + 1).astype(F32)).astype(BF16)
        source[...] = dot_rows(src_in[...], onto)

    with jax.named_scope("send1"):
        pair_wait(1, 1)
        send_step(1)
    with jax.named_scope("rs0"):
        pieces(0)
    with jax.named_scope("rimwait"):
        rim_copy(0, rim - 1, 1).wait()
    with jax.named_scope("rim23"):
        for q in range(rim - 1):
            turn_rim(q)
        lax.fori_loop(0, rim, last_steps_rim, 0)
        pair_copy(2, steps - 2, 2).start()
    with jax.named_scope("send23"):
        pair_wait(2, steps - 2)
        for s in range(2, steps):
            send_step(s)
    with jax.named_scope("rs1"):
        pieces(1)

    def place_of(i):
        return HALF * 2 if i == HALF else i - (i > HALF)

    def terms_rows(i, first, count):
        return pl.ds(i * shots + first, count)

    def ch_copy(n, i, g):
        return remote(csend.at[n - 1, terms_rows(i, g * group, group)], cgot.at[n - 1, g, place_of(i)], ch_ss, ch_rs.at[n - 1, g], patch_at(i - HALF), 0)

    def out_copy(i, lag):
        return remote(csend.at[last - 1, terms_rows(i, lag * chunk, chunk)], cbuf.at[place_of(i)], out_ss, out_rs, patch_at(i - HALF), lag)

    def spread_copy(s, part, lag):
        rows = pl.ds(part * chunk, chunk)
        return remote(dens.at[s, rows], dens.at[s, rows], sp_ss, ag_rs if part == 0 else sp_rs.at[s], t, lag)

    def others(d):
        return pl.when(lag_at(d) != 0)

    def new_terms(k, s, i, rows):
        return is_active(k, i) * dot(dens[s, rows, :], w_buf[k - 1, :, pl.ds(i * width, width)])

    def send_terms(n, g):
        rows = pl.ds(g * group, group)
        for i in (0, NEAR - 1, 1, NEAR - 2, *range(2, NEAR - 2)):
            value = new_terms(1, n - 1, i, rows)
            if n > 1:
                value = value + cacc[n - 2, i, rows, :]
            csend[n - 1, terms_rows(i, g * group, group), :] = value.astype(BF16)
            if n < last:
                if i != HALF:
                    ch_copy(n, i, g).start()
            else:
                for lag in range(g * group // chunk, (g + 1) * group // chunk):
                    if i == HALF and lag == 0:
                        cbuf[place_of(i)] = value[:chunk].astype(BF16)
                    else:
                        out_copy(i, lag).start()

    def older_terms(s):
        for n in range(s + 2, steps):
            for i in range(NEAR):
                value = new_terms(n - s, s, i, pl.ds(0, shots))
                if s > 0:
                    value = value + cacc[n - 2, i]
                cacc[n - 2, i] = value

    def finish(n, g):
        rest = -piece_sum(n, g * group, group) - csend[n - 1, terms_rows(HALF, g * group, group), :].astype(F32)
        landed(cgot.at[n - 1, g], ch_rs.at[n - 1, g])
        for i in range(NEAR - 1):
            rest = rest - cgot[n - 1, g, i].astype(F32)
        dens[n, pl.ds(g * group, group), :] = density_of(rest)

    def spread(s):
        for lag in range(1, lags):
            spread_copy(s, lag, lag).start()
            spread_copy(s, 0, lag).start()

    @pl.when(is_first)
    def _():
        with jax.named_scope("p0"):
            piece_wait(0)
        with jax.named_scope("terms1"):
            dens[0] = density_of(-piece_sum(0, 0, shots))
            for g in range(groups):
                send_terms(1, g)
            spread(0)
        with jax.named_scope("older1"):
            older_terms(0)
        with jax.named_scope("rs2"):
            pieces(2)
        with jax.named_scope("rs3"):
            own_last[...] = last_sum()
        for n in range(1, last):
            with jax.named_scope(f"p{n}"):
                piece_wait(n)
            for g in range(groups):
                with jax.named_scope(f"finish{n}{g}"):
                    finish(n, g)
                with jax.named_scope(f"terms{n + 1}{g}"):
                    send_terms(n + 1, g)
            spread(n)
            with jax.named_scope(f"older{n + 1}"):
                older_terms(n)

    @pl.when(l != 0)
    def _():
        with jax.named_scope("rs2"):
            pieces(2)
        with jax.named_scope("rs3"):
            own_last[...] = last_sum()
        with jax.named_scope("sp"):
            for n in range(last):
                landed(dens.at[n, own_shots], sp_rs.at[n])
                for d in range(1, lags):
                    others(d)(ag_copy(n, d, pass_ss).start)

    with jax.named_scope("nblast"):
        rest = -nb_sum(own_last[...])
    with jax.named_scope("outwait"):
        @pl.when(is_first)
        def _():
            landed(cbuf.at[pl.ds(0, NEAR - 1)], out_rs)

        @pl.when(l != 0)
        def _():
            landed(cbuf, out_rs)

        for i in range(NEAR):
            rest = rest - cbuf[i].astype(F32)
    with jax.named_scope("dlast"):
        dens[last, own_shots, :] = density_of(rest)
        for d in range(1, lags):
            ag_copy(last, d, ag_ss).start()

    with jax.named_scope("aglast"):
        seven = pl.ds(0, (lags - 1) * chunk)

        @pl.when(is_first)
        def _():
            landed(dens.at[0, seven], ag_rs)

        @pl.when(l != 0)
        def _():
            landed(dens.at[:, seven], ag_rs)

    with jax.named_scope("fin"):
        for s in range(steps):
            out_ref[s] = dens[s].T
        landed(src_in.at[pl.ds(0, (patches - 1) * CAP)], src_ss)
        landed(rbuf.at[:, pl.ds(0, lags - 1)], rs_ss)
        landed(got, pair_ss)
        landed(nbuf, nb_ss)
        landed(dens.at[0, seven], ag_ss)

        @pl.when(is_first)
        def _():
            landed(pbuf.at[:, pl.ds(0, HALF * chunk)], p_ss)
            landed(cgot, ch_ss)
            landed(csend.at[last - 1, pl.ds(0, (NEAR * lags - 1) * chunk)], out_ss)
            landed(pbuf.at[:, pl.ds(0, 2 * (lags - 1) * chunk)], sp_ss)

        @pl.when(l != 0)
        def _():
            landed(pbuf.at[:, pl.ds(0, (HALF + 1) * chunk)], p_ss)
            landed(dens.at[pl.ds(0, last), pl.ds(0, (lags - 2) * chunk)], pass_ss)


def local(patches, lags, interaction, history, near_inverse, lag_ranges, receiver_tile, receiver_panel, residuals):
    band, width, cols = interaction.shape
    shots = history.shape[2]
    recv, steps, _ = residuals.shape
    chunk = shots // lags
    src_width = -(-(steps * chunk + 1) // 128) * 128
    per = 3 if band % 3 == 0 else 1
    any_space = pl.BlockSpec(memory_space=pl.ANY)
    vmem = pl.BlockSpec(memory_space=pltpu.VMEM)
    dma = pltpu.SemaphoreType.DMA
    out = pl.pallas_call(
        functools.partial(kernel, patches, lags),
        out_shape=jax.ShapeDtypeStruct((steps, width, shots), BF16),
        in_specs=[any_space, any_space, any_space, pl.BlockSpec(memory_space=pltpu.SMEM), vmem, vmem, any_space],
        out_specs=vmem,
        scratch_shapes=[
            pltpu.VMEM((band, width, cols), BF16),
            pltpu.VMEM((band, width, shots), BF16),
            pltpu.VMEM(near_inverse.shape, BF16),
            pltpu.VMEM((recv, steps, shots), BF16),
            pltpu.VMEM((steps - 1, width, shots), BF16),
            pltpu.VMEM(((band + steps - 1) * shots, width), BF16),
            pltpu.VMEM((steps * shots, cols), F32),
            pltpu.VMEM((steps * shots, HALF * width), F32),
            pltpu.VMEM((steps, shots, (HALF + 1) * width), BF16),
            pltpu.VMEM((steps, lags, chunk, (HALF + 1) * width), BF16),
            pltpu.VMEM((steps - 1, HALF + 1, chunk, width), BF16),
            pltpu.VMEM((steps - 1, chunk, width), BF16),
            pltpu.VMEM((steps - 1, (HALF + 1) * shots, width), BF16),
            pltpu.VMEM((HALF + 1, chunk, width), F32),
            pltpu.VMEM((2, chunk, width), F32),
            pltpu.VMEM((chunk, width), F32),
            pltpu.VMEM((patches * CAP, src_width), BF16),
            pltpu.VMEM((patches * CAP, src_width), BF16),
            pltpu.VMEM((src_width, width), F32),
            pltpu.VMEM((steps, shots, width), BF16),
            pltpu.VMEM((steps - 2, NEAR, shots, width), F32),
            pltpu.VMEM((steps - 1, NEAR * shots, width), BF16),
            pltpu.VMEM((steps - 2, GROUPS, NEAR - 1, shots // GROUPS, width), BF16),
            pltpu.VMEM((NEAR, chunk, width), BF16),
            dma((band // per,)), dma, dma, dma, dma((2,)), dma((2,)), dma, dma, dma, dma((steps,)), dma, dma((steps - 1,)), dma, dma,
            dma, dma, dma, dma, dma((3,)), dma, dma((steps - 2, GROUPS)), dma, dma, dma, dma((steps - 1,)),
        ],
        compiler_params=pltpu.CompilerParams(collective_id=0, has_side_effects=True, vmem_limit_bytes=60 * 1024 * 1024),
        name="march",
    )(
        interaction, history, near_inverse, lag_ranges, receiver_tile.reshape(1, recv), receiver_panel.reshape(1, recv),
        residuals,
    )
    return out


def solution(mesh):
    in_specs = (
        P("lag", "patch", None),
        P("lag", "patch", None),
        P("patch", None),
        P("patch", None),
        P("patch", None),
        P("patch"),
        P("patch", None, None),
    )
    body = functools.partial(local, mesh.shape["patch"], mesh.shape["lag"])
    return jax.shard_map(body, mesh=mesh, in_specs=in_specs, out_specs=P(None, "patch", None), check_vma=False)
```

```python
import functools

import jax
import jax.numpy as jnp
from jax import lax
from jax.experimental import pallas as pl
from jax.experimental.pallas import tpu as pltpu
from jax.sharding import PartitionSpec as P

NEAR = 5
HALF = NEAR // 2
CAP = 16
GROUPS = 2
MESH = pl.DeviceIdType.MESH
F32 = jnp.float32
BF16 = jnp.bfloat16


def remote(src, dst, send, recv, patch, lag):
    return pltpu.make_async_remote_copy(
        src_ref=src,
        dst_ref=dst,
        send_sem=send,
        recv_sem=recv,
        device_id={"patch": patch, "lag": lag},
        device_id_type=MESH,
    )


def landed(region, sem):
    pltpu.make_async_copy(region, region, sem).wait()


def dot(a, b):
    return jnp.dot(a, b, preferred_element_type=F32)


def dot_rows(a, b):
    return lax.dot_general(a, b, (((0,), (0,)), ((), ())), preferred_element_type=F32)


def iota(shape, dim):
    return lax.broadcasted_iota(jnp.int32, shape, dim)


def kernel(
    patches, lags, w_hbm, h_hbm, inv_hbm, range_ref, tile_ref, panel_ref, resid_hbm, out_ref,
    w_buf, h_buf, inv_ref, resid_ref, rim_buf, ht, acc, got, sbuf, rbuf, psend, own_send, pbuf, nsend, nbuf, own_last, src_out, src_in, source, dens, cacc, csend, cgot, cbuf,
    w_sem, h_sem, inv_sem, resid_sem, rim_ss, rim_rs, src_ss, src_rs, rs_ss, rs_rs, p_ss, p_rs, nb_ss, nb_rs,
    ag_ss, ag_rs, pass_ss, pair_ss, pair_rs, ch_ss, ch_rs, out_ss, out_rs, sp_ss, sp_rs,
):
    t, l = lax.axis_index("patch"), lax.axis_index("lag")
    band, width, cols = w_buf.shape
    core = lax.rem(t, 2)
    given, kept = HALF * width, (HALF + 1) * width
    steps, shots, _ = sbuf.shape
    chunk = shots // lags
    rim = steps - 1
    groups = GROUPS
    group = shots // groups
    is_first = l == 0

    def patch_at(d):
        return lax.rem(t + d + patches, patches)

    def lag_at(d):
        return lax.rem(l + d, lags)

    resid_copy = pltpu.make_async_copy(resid_hbm, resid_ref, resid_sem)
    resid_copy.start()
    h_copy = pltpu.make_async_copy(h_hbm, h_buf, h_sem)
    h_copy.start()
    inv_copy = pltpu.make_async_copy(inv_hbm, inv_ref, inv_sem)

    per = band // w_sem.shape[0]

    def w_copy(a):
        lags_of = pl.ds(a * per, per)
        return pltpu.make_async_copy(w_hbm.at[lags_of], w_buf.at[lags_of], w_sem.at[a])

    w_copy(0).start()

    barrier = pltpu.get_barrier_semaphore()

    def greet(patch, lag):
        pl.semaphore_signal(barrier, inc=1, device_id={"patch": patch, "lag": lag}, device_id_type=MESH)

    for d in range(1, lags):
        greet(t, lag_at(d))

    def greet_patch(d, carry):
        greet(patch_at(d), l)
        return carry

    lax.fori_loop(1, patches, greet_patch, 0)
    near_by = [d for d in range(-HALF, HALF + 1) if d != 0]

    @pl.when(is_first)
    def _():
        for d in near_by:
            for other in range(1, lags):
                greet(patch_at(d), other)

    @pl.when(l != 0)
    def _():
        for d in near_by:
            greet(patch_at(d), 0)

    def turn(j, carry):
        ht[pl.ds(pl.multiple_of((band - 1 - j) * shots, shots), shots), :] = h_buf[j].T
        return carry

    with jax.named_scope("turn"):
        h_copy.wait()
        for a in range(1, band // per):
            w_copy(a).start()
        inv_copy.start()
        lax.fori_loop(0, band, turn, 0)

    def is_active(lag_number, i):
        low, high = range_ref[0, i], range_ref[0, NEAR + i]
        return jnp.where((lag_number >= low) & (lag_number < high), 1.0, 0.0).astype(F32)

    def patch_block(q):
        return q + (HALF + 1) * (1 - core) if q < HALF else q - HALF + HALF * core

    def lag_terms(j, q, first_row, rows):
        i = patch_block(q)
        left = ht[pl.ds(pl.multiple_of((band - 1 - j) * shots + first_row, shots), rows), :]
        right = w_buf[j, :, pl.ds(pl.multiple_of(i * width, width), width)]
        return is_active(l * band + j + 1, i) * dot(left, right)

    def add_lag(j, first_row, rows):
        for q in range(NEAR):
            acc[pl.ds(first_row, rows), pl.ds(q * width, width)] += lag_terms(j, q, first_row, rows)

    def set_lag(j, first_row, rows):
        for q in range(NEAR):
            acc[pl.ds(first_row, rows), pl.ds(q * width, width)] = lag_terms(j, q, first_row, rows)

    def pair_copy(first, count, at):
        rows = pl.ds(first * shots, count * shots)
        return remote(acc.at[rows, pl.ds(0, given)], got.at[rows], pair_ss, pair_rs.at[at], t + 1 - 2 * core, l)

    def pair_wait(first, count):
        landed(got.at[pl.ds(first * shots, count * shots)], pair_rs.at[min(first, 2)])

    def first_step(j, carry):
        add_lag(j, 0, shots)
        return carry

    def later_steps(j, carry):
        add_lag(j, shots, (steps - 1) * shots)
        return carry

    def second_step_rim(j, carry):
        add_lag(j, shots, shots)
        return carry

    def last_steps_rim(j, carry):
        add_lag(j, 2 * shots, (steps - 2) * shots)
        return carry

    def rim_copy(first, count, at):
        return remote(h_buf.at[pl.ds(band - rim + first, count)], rim_buf.at[pl.ds(first, count)], rim_ss.at[at], rim_rs.at[at], t, lag_at(1))

    def rim_start(first, count, at):
        pl.when(l != lags - 1)(rim_copy(first, count, at).start)

    def rim_take(first, count, at):
        rows = pl.ds((band + rim - first - count) * shots, count * shots)

        @pl.when(is_first)
        def _():
            ht[rows, :] = jnp.zeros((count * shots, width), BF16)

        @pl.when(l != 0)
        def _():
            landed(rim_buf.at[pl.ds(first, count)], rim_rs.at[at])
            for q in range(first, first + count):
                ht[pl.ds((band + rim - 1 - q) * shots, shots), :] = rim_buf[q].T

    def slots(p):
        return pl.ds(pl.multiple_of(p * CAP, CAP), CAP)

    own_slots = pl.ds(pl.multiple_of(t * CAP, CAP), CAP)

    def src_copy(d):
        to = patch_at(d)
        return remote(src_out.at[slots(to)], src_in.at[own_slots], src_ss, src_rs, to, l)

    def src_start(d, carry):
        src_copy(d).start()
        return carry

    def rs_copy(s, d):
        to = lag_at(d)
        part = pl.ds(pl.multiple_of(to * chunk, chunk), chunk)
        return remote(sbuf.at[s, part], rbuf.at[s, l], rs_ss, rs_rs.at[s], t, to)

    def send_step(s):
        rows = pl.ds(s * shots, shots)
        shared = pl.ds(pl.multiple_of(given + width * (1 - core), width), given)
        acc[rows, shared] += got[rows, :]
        sbuf[s] = acc[rows, pl.ds(given, kept)].astype(BF16)
        for d in range(1, lags):
            rs_copy(s, d).start()

    own_shots = pl.ds(pl.multiple_of(l * chunk, chunk), chunk)

    last = steps - 1

    def lag_sum(s):
        total = acc[pl.ds(pl.multiple_of(s * shots + l * chunk, chunk), chunk), pl.ds(given, kept)]
        landed(rbuf.at[s, pl.ds(0, lags - 1)], rs_rs.at[s])
        for d in range(1, lags):
            total = total + rbuf[s, lag_at(d)].astype(F32)
        parts = [total[:, m * width : (m + 1) * width] for m in range(HALF + 1)]
        own = jnp.where(core == 0, parts[HALF], parts[0]) - source[pl.ds(s * chunk, chunk), :]
        return parts, own

    def owner(f):
        return patch_at(f - HALF + (HALF + 1) * core)

    def piece_rows(side, lag):
        return pl.ds(pl.multiple_of(side * shots + lag * chunk, chunk), chunk)

    def piece_copy(s, f):
        return remote(psend.at[s, f + core], pbuf.at[s, piece_rows(HALF - core, l)], p_ss, p_rs.at[s], owner(f), 0)

    def own_piece_copy(s):
        return remote(own_send.at[s], pbuf.at[s, piece_rows(0, l)], p_ss, p_rs.at[s], t, 0)

    def pieces(s):
        parts, own = lag_sum(s)
        for m in range(HALF + 1):
            psend[s, m] = parts[m].astype(BF16)
        for f in range(HALF):
            piece_copy(s, f).start()

        @pl.when(is_first)
        def _():
            pbuf[s, pl.ds(0, chunk), :] = own.astype(BF16)

        @pl.when(l != 0)
        def _():
            own_send[s] = own.astype(BF16)
            own_piece_copy(s).start()

    def piece_wait(s):
        landed(pbuf.at[s, pl.ds(chunk, (HALF + 1) * shots - chunk)], p_rs.at[s])

    def piece_sum(s, first, count):
        sides = [pbuf[s, pl.ds(side * shots + first, count), :].astype(F32) for side in range(HALF + 1)]
        return sides[0] + sides[1] + sides[2]

    def nb_copy(f):
        return remote(nsend.at[f + core], nbuf.at[1 - core], nb_ss, nb_rs, owner(f), l)

    def last_sum():
        parts, own = lag_sum(last)
        for m in range(HALF + 1):
            nsend[m] = parts[m]
        for f in range(HALF):
            nb_copy(f).start()
        return own

    def nb_sum(own):
        landed(nbuf, nb_rs)
        return own + nbuf[0] + nbuf[1]

    def density_of(right):
        return dot(right.astype(BF16), inv_ref[...]).astype(BF16)

    def ag_copy(s, d, sent):
        return remote(dens.at[s, own_shots], dens.at[s, own_shots], sent, ag_rs, t, lag_at(d))

    with jax.named_scope("first"):
        w_copy(0).wait()
        set_lag(0, 0, shots)
        lax.fori_loop(1, per, first_step, 0)
        for a in range(1, band // per):
            w_copy(a).wait()
            lax.fori_loop(a * per, (a + 1) * per, first_step, 0)
    with jax.named_scope("bar"):
        pl.semaphore_wait(barrier, jnp.where(is_first, lags - 1 + patches - 1 + 4 * (lags - 1), lags - 1 + patches - 1 + 4))
    with jax.named_scope("pair0"):
        pair_copy(0, 1, 0).start()
        rim_start(rim - 1, 1, 0)

    with jax.named_scope("prep"):
        recv = tile_ref.shape[1]
        diagonal = iota((recv, recv), 0) == iota((recv, recv), 1)

        def as_column(row):
            return jnp.sum(jnp.where(diagonal, row.astype(F32), 0.0), axis=1, keepdims=True)

        tile_col = as_column(tile_ref[...])
        panel_col = as_column(panel_ref[...])
        named = (tile_col == iota((recv, 128), 1).astype(F32)).astype(F32)
        earlier = (iota((recv, recv), 1) < iota((recv, recv), 0)).astype(BF16)
        rank = jnp.sum(dot(earlier, named.astype(BF16)) * named, axis=1, keepdims=True)
        slot = tile_col * CAP + rank
        placer = (slot == iota((recv, patches * CAP), 1).astype(F32)).astype(BF16)
        src_width = src_out.shape[1]
        mine = jnp.zeros((recv, src_width), F32)
        resid_copy.wait()
        for s in range(steps):
            lane, place = iota((shots, src_width), 0), iota((shots, src_width), 1)
            pick = (lane - l * chunk == place - s * chunk) & (place >= s * chunk) & (place < (s + 1) * chunk)
            mine = mine + dot(resid_ref[:, s, :], pick.astype(BF16))
        mine = jnp.where(iota((recv, src_width), 1) == steps * chunk, panel_col + 1.0, mine).astype(BF16)
        src_out[...] = dot_rows(placer, mine).astype(BF16)
        src_in[own_slots, :] = src_out[own_slots, :]

    with jax.named_scope("pairwait0"):
        pair_wait(0, 1)
    with jax.named_scope("send0"):
        send_step(0)
        lax.fori_loop(1, patches, src_start, 0)
        rim_start(0, rim - 1, 1)
    with jax.named_scope("later2"):
        set_lag(rim, shots, (steps - 1) * shots)
        lax.fori_loop(rim + 1, band, later_steps, 0)

    with jax.named_scope("rim1"):
        rim_take(rim - 1, 1, 0)
        lax.fori_loop(0, rim, second_step_rim, 0)
        pair_copy(1, 1, 1).start()

    with jax.named_scope("srcwait"):
        landed(src_in.at[pl.ds(0, (patches - 1) * CAP)], src_rs)
        inv_copy.wait()
    with jax.named_scope("src"):
        labels = src_in[:, pl.ds(steps * chunk, 1)].astype(F32)
        onto = (labels == (iota((patches * CAP, width), 1) + 1).astype(F32)).astype(BF16)
        source[...] = dot_rows(src_in[...], onto)

    with jax.named_scope("rs0"):
        pieces(0)
    with jax.named_scope("send1"):
        pair_wait(1, 1)
        send_step(1)
    with jax.named_scope("rim23"):
        rim_take(0, rim - 1, 1)
        lax.fori_loop(0, rim, last_steps_rim, 0)
        pair_copy(2, steps - 2, 2).start()
    with jax.named_scope("send2"):
        pair_wait(2, steps - 2)
        send_step(2)

    def place_of(i):
        return HALF * 2 if i == HALF else i - (i > HALF)

    def terms_rows(i, first, count):
        return pl.ds(i * shots + first, count)

    def ch_copy(n, i, g):
        return remote(csend.at[n - 1, terms_rows(i, g * group, group)], cgot.at[n - 1, g, place_of(i)], ch_ss, ch_rs.at[n - 1, g], patch_at(i - HALF), 0)

    def out_copy(i, lag):
        return remote(csend.at[last - 1, terms_rows(i, lag * chunk, chunk)], cbuf.at[place_of(i)], out_ss, out_rs, patch_at(i - HALF), lag)

    def spread_copy(s, part, lag):
        rows = pl.ds(part * chunk, chunk)
        return remote(dens.at[s, rows], dens.at[s, rows], sp_ss, ag_rs if part == 0 else sp_rs.at[s], t, lag)

    def others(d):
        return pl.when(lag_at(d) != 0)

    def new_terms(k, s, i, rows):
        return is_active(k, i) * dot(dens[s, rows, :], w_buf[k - 1, :, pl.ds(i * width, width)])

    def send_terms(n, g):
        rows = pl.ds(g * group, group)
        for i in (0, NEAR - 1, 1, NEAR - 2, *range(2, NEAR - 2)):
            value = new_terms(1, n - 1, i, rows)
            if n > 1:
                value = value + cacc[n - 2, i, rows, :]
            csend[n - 1, terms_rows(i, g * group, group), :] = value.astype(BF16)
            if n < last:
                if i != HALF:
                    ch_copy(n, i, g).start()
            else:
                for lag in range(g * group // chunk, (g + 1) * group // chunk):
                    if i == HALF and lag == 0:
                        cbuf[place_of(i)] = value[:chunk].astype(BF16)
                    else:
                        out_copy(i, lag).start()

    def older_terms(s):
        for n in range(s + 2, steps):
            for i in range(NEAR):
                value = new_terms(n - s, s, i, pl.ds(0, shots))
                if s > 0:
                    value = value + cacc[n - 2, i]
                cacc[n - 2, i] = value

    def finish(n, g):
        rest = -piece_sum(n, g * group, group) - csend[n - 1, terms_rows(HALF, g * group, group), :].astype(F32)
        landed(cgot.at[n - 1, g], ch_rs.at[n - 1, g])
        for i in range(NEAR - 1):
            rest = rest - cgot[n - 1, g, i].astype(F32)
        dens[n, pl.ds(g * group, group), :] = density_of(rest)

    def spread(s):
        for lag in range(1, lags):
            spread_copy(s, lag, lag).start()
            spread_copy(s, 0, lag).start()

    @pl.when(is_first)
    def _():
        with jax.named_scope("rs1"):
            pieces(1)
        with jax.named_scope("p0"):
            piece_wait(0)
        with jax.named_scope("terms1"):
            dens[0] = density_of(-piece_sum(0, 0, shots))
            for g in range(groups):
                send_terms(1, g)
            spread(0)
        with jax.named_scope("older1"):
            older_terms(0)
        with jax.named_scope("rs2"):
            pieces(2)
        with jax.named_scope("send3"):
            send_step(last)
        for n in range(1, last):
            with jax.named_scope(f"p{n}"):
                piece_wait(n)
            for g in range(groups):
                with jax.named_scope(f"finish{n}{g}"):
                    finish(n, g)
                with jax.named_scope(f"terms{n + 1}{g}"):
                    send_terms(n + 1, g)
            spread(n)
            if n == 1:
                with jax.named_scope("older2"):
                    older_terms(n)
                with jax.named_scope("rs3"):
                    own_last[...] = last_sum()

    @pl.when(l != 0)
    def _():
        def pass_on(n):
            landed(dens.at[n, own_shots], sp_rs.at[n])
            for d in range(1, lags):
                others(d)(ag_copy(n, d, pass_ss).start)

        with jax.named_scope("rs1"):
            pieces(1)
        with jax.named_scope("rs2"):
            pieces(2)
        with jax.named_scope("sp0"):
            pass_on(0)
        with jax.named_scope("send3"):
            send_step(last)
        with jax.named_scope("rs3"):
            own_last[...] = last_sum()
        with jax.named_scope("sp"):
            for n in range(1, last):
                pass_on(n)

    with jax.named_scope("nblast"):
        rest = -nb_sum(own_last[...])
    with jax.named_scope("outwait"):
        @pl.when(is_first)
        def _():
            landed(cbuf.at[pl.ds(0, NEAR - 1)], out_rs)

        @pl.when(l != 0)
        def _():
            landed(cbuf, out_rs)

        for i in range(NEAR):
            rest = rest - cbuf[i].astype(F32)
    with jax.named_scope("dlast"):
        dens[last, own_shots, :] = density_of(rest)
        for d in range(1, lags):
            ag_copy(last, d, ag_ss).start()

    with jax.named_scope("aglast"):
        seven = pl.ds(0, (lags - 1) * chunk)

        @pl.when(is_first)
        def _():
            landed(dens.at[0, seven], ag_rs)

        @pl.when(l != 0)
        def _():
            landed(dens.at[:, seven], ag_rs)

    with jax.named_scope("fin"):
        for s in range(steps):
            out_ref[s] = dens[s].T
        landed(src_in.at[pl.ds(0, (patches - 1) * CAP)], src_ss)

        @pl.when(l != lags - 1)
        def _():
            landed(rim_buf.at[pl.ds(rim - 1, 1)], rim_ss.at[0])
            landed(rim_buf.at[pl.ds(0, rim - 1)], rim_ss.at[1])

        landed(rbuf.at[:, pl.ds(0, lags - 1)], rs_ss)
        landed(got, pair_ss)
        landed(nbuf, nb_ss)
        landed(dens.at[0, seven], ag_ss)

        @pl.when(is_first)
        def _():
            landed(pbuf.at[:, pl.ds(0, HALF * chunk)], p_ss)
            landed(cgot, ch_ss)
            landed(csend.at[last - 1, pl.ds(0, (NEAR * lags - 1) * chunk)], out_ss)
            landed(pbuf.at[:, pl.ds(0, 2 * (lags - 1) * chunk)], sp_ss)

        @pl.when(l != 0)
        def _():
            landed(pbuf.at[:, pl.ds(0, (HALF + 1) * chunk)], p_ss)
            landed(dens.at[pl.ds(0, last), pl.ds(0, (lags - 2) * chunk)], pass_ss)


def local(patches, lags, interaction, history, near_inverse, lag_ranges, receiver_tile, receiver_panel, residuals):
    band, width, cols = interaction.shape
    shots = history.shape[2]
    recv, steps, _ = residuals.shape
    chunk = shots // lags
    src_width = -(-(steps * chunk + 1) // 128) * 128
    per = 3 if band % 3 == 0 else 1
    any_space = pl.BlockSpec(memory_space=pl.ANY)
    vmem = pl.BlockSpec(memory_space=pltpu.VMEM)
    dma = pltpu.SemaphoreType.DMA
    out = pl.pallas_call(
        functools.partial(kernel, patches, lags),
        out_shape=jax.ShapeDtypeStruct((steps, width, shots), BF16),
        in_specs=[any_space, any_space, any_space, pl.BlockSpec(memory_space=pltpu.SMEM), vmem, vmem, any_space],
        out_specs=vmem,
        scratch_shapes=[
            pltpu.VMEM((band, width, cols), BF16),
            pltpu.VMEM((band, width, shots), BF16),
            pltpu.VMEM(near_inverse.shape, BF16),
            pltpu.VMEM((recv, steps, shots), BF16),
            pltpu.VMEM((steps - 1, width, shots), BF16),
            pltpu.VMEM(((band + steps - 1) * shots, width), BF16),
            pltpu.VMEM((steps * shots, cols), F32),
            pltpu.VMEM((steps * shots, HALF * width), F32),
            pltpu.VMEM((steps, shots, (HALF + 1) * width), BF16),
            pltpu.VMEM((steps, lags, chunk, (HALF + 1) * width), BF16),
            pltpu.VMEM((steps - 1, HALF + 1, chunk, width), BF16),
            pltpu.VMEM((steps - 1, chunk, width), BF16),
            pltpu.VMEM((steps - 1, (HALF + 1) * shots, width), BF16),
            pltpu.VMEM((HALF + 1, chunk, width), F32),
            pltpu.VMEM((2, chunk, width), F32),
            pltpu.VMEM((chunk, width), F32),
            pltpu.VMEM((patches * CAP, src_width), BF16),
            pltpu.VMEM((patches * CAP, src_width), BF16),
            pltpu.VMEM((src_width, width), F32),
            pltpu.VMEM((steps, shots, width), BF16),
            pltpu.VMEM((steps - 2, NEAR, shots, width), F32),
            pltpu.VMEM((steps - 1, NEAR * shots, width), BF16),
            pltpu.VMEM((steps - 2, GROUPS, NEAR - 1, shots // GROUPS, width), BF16),
            pltpu.VMEM((NEAR, chunk, width), BF16),
            dma((band // per,)), dma, dma, dma, dma((2,)), dma((2,)), dma, dma, dma, dma((steps,)), dma, dma((steps - 1,)), dma, dma,
            dma, dma, dma, dma, dma((3,)), dma, dma((steps - 2, GROUPS)), dma, dma, dma, dma((steps - 1,)),
        ],
        compiler_params=pltpu.CompilerParams(collective_id=0, has_side_effects=True, vmem_limit_bytes=60 * 1024 * 1024),
        name="march",
    )(
        interaction, history, near_inverse, lag_ranges, receiver_tile.reshape(1, recv), receiver_panel.reshape(1, recv),
        residuals,
    )
    return out


def solution(mesh):
    in_specs = (
        P("lag", "patch", None),
        P("lag", "patch", None),
        P("patch", None),
        P("patch", None),
        P("patch", None),
        P("patch"),
        P("patch", None, None),
    )
    body = functools.partial(local, mesh.shape["patch"], mesh.shape["lag"])
    return jax.shard_map(body, mesh=mesh, in_specs=in_specs, out_specs=P(None, "patch", None), check_vma=False)
```

```python
import functools

import jax
import jax.numpy as jnp
from jax import lax
from jax.experimental import pallas as pl
from jax.experimental.pallas import tpu as pltpu
from jax.sharding import PartitionSpec as P

NEAR = 5
HALF = NEAR // 2
CAP = 16
GROUPS = 2
MESH = pl.DeviceIdType.MESH
F32 = jnp.float32
BF16 = jnp.bfloat16


def remote(src, dst, send, recv, patch, lag):
    return pltpu.make_async_remote_copy(
        src_ref=src,
        dst_ref=dst,
        send_sem=send,
        recv_sem=recv,
        device_id={"patch": patch, "lag": lag},
        device_id_type=MESH,
    )


def landed(region, sem):
    pltpu.make_async_copy(region, region, sem).wait()


def dot(a, b):
    return jnp.dot(a, b, preferred_element_type=F32)


def dot_rows(a, b):
    return lax.dot_general(a, b, (((0,), (0,)), ((), ())), preferred_element_type=F32)


def iota(shape, dim):
    return lax.broadcasted_iota(jnp.int32, shape, dim)


def kernel(
    patches, lags, w_hbm, h_hbm, inv_hbm, range_ref, tile_ref, panel_ref, resid_hbm, out_ref,
    w_buf, h_buf, inv_ref, resid_ref, rim_buf, ht, acc, got, sbuf, rbuf, psend, own_send, pbuf, nsend, nbuf, own_last, src_out, src_in, source, dens, cacc, csend, cgot, cbuf,
    w_sem, h_sem, inv_sem, resid_sem, rim_ss, rim_rs, src_ss, src_rs, rs_ss, rs_rs, p_ss, p_rs, nb_ss, nb_rs,
    ag_ss, ag_rs, pass_ss, pair_ss, pair_rs, ch_ss, ch_rs, out_ss, out_rs, sp_ss, sp_rs,
):
    t, l = lax.axis_index("patch"), lax.axis_index("lag")
    band, width, cols = w_buf.shape
    core = lax.rem(t, 2)
    given, kept = HALF * width, (HALF + 1) * width
    steps, shots, _ = sbuf.shape
    chunk = shots // lags
    rim = steps - 1
    groups = GROUPS
    group = shots // groups
    is_first = l == 0

    def patch_at(d):
        return lax.rem(t + d + patches, patches)

    def lag_at(d):
        return lax.rem(l + d, lags)

    resid_copy = pltpu.make_async_copy(resid_hbm, resid_ref, resid_sem)
    resid_copy.start()
    h_copy = pltpu.make_async_copy(h_hbm, h_buf, h_sem)
    h_copy.start()
    inv_copy = pltpu.make_async_copy(inv_hbm, inv_ref, inv_sem)

    per = band // w_sem.shape[0]

    def w_copy(a):
        lags_of = pl.ds(a * per, per)
        return pltpu.make_async_copy(w_hbm.at[lags_of], w_buf.at[lags_of], w_sem.at[a])

    w_copy(0).start()

    barrier = pltpu.get_barrier_semaphore()

    def greet(patch, lag):
        pl.semaphore_signal(barrier, inc=1, device_id={"patch": patch, "lag": lag}, device_id_type=MESH)

    for d in range(1, lags):
        greet(t, lag_at(d))

    def greet_patch(d, carry):
        greet(patch_at(d), l)
        return carry

    lax.fori_loop(1, patches, greet_patch, 0)
    near_by = [d for d in range(-HALF, HALF + 1) if d != 0]

    @pl.when(is_first)
    def _():
        for d in near_by:
            for other in range(1, lags):
                greet(patch_at(d), other)

    @pl.when(l != 0)
    def _():
        for d in near_by:
            greet(patch_at(d), 0)

    def turn(j, carry):
        ht[pl.ds(pl.multiple_of((band - 1 - j) * shots, shots), shots), :] = h_buf[j].T
        return carry

    with jax.named_scope("turn"):
        h_copy.wait()
        for a in range(1, band // per):
            w_copy(a).start()
        inv_copy.start()
        lax.fori_loop(0, band, turn, 0)

    def is_active(lag_number, i):
        low, high = range_ref[0, i], range_ref[0, NEAR + i]
        return jnp.where((lag_number >= low) & (lag_number < high), 1.0, 0.0).astype(F32)

    def patch_block(q):
        return q + (HALF + 1) * (1 - core) if q < HALF else q - HALF + HALF * core

    def lag_terms(j, q, first_row, rows):
        i = patch_block(q)
        left = ht[pl.ds(pl.multiple_of((band - 1 - j) * shots + first_row, shots), rows), :]
        right = w_buf[j, :, pl.ds(pl.multiple_of(i * width, width), width)]
        return is_active(l * band + j + 1, i) * dot(left, right)

    def add_lag(j, first_row, rows):
        for q in range(NEAR):
            acc[pl.ds(first_row, rows), pl.ds(q * width, width)] += lag_terms(j, q, first_row, rows)

    def set_lag(j, first_row, rows):
        for q in range(NEAR):
            acc[pl.ds(first_row, rows), pl.ds(q * width, width)] = lag_terms(j, q, first_row, rows)

    def pair_copy(first, count, at):
        rows = pl.ds(first * shots, count * shots)
        return remote(acc.at[rows, pl.ds(0, given)], got.at[rows], pair_ss, pair_rs.at[at], t + 1 - 2 * core, l)

    def pair_wait(first, count):
        landed(got.at[pl.ds(first * shots, count * shots)], pair_rs.at[min(first, 2)])

    def first_step(j, carry):
        add_lag(j, 0, shots)
        return carry

    def later_steps(j, carry):
        add_lag(j, shots, (steps - 1) * shots)
        return carry

    def second_step_rim(j, carry):
        add_lag(j, shots, shots)
        return carry

    def last_steps_rim(j, carry):
        add_lag(j, 2 * shots, (steps - 2) * shots)
        return carry

    def rim_copy(first, count, at):
        return remote(h_buf.at[pl.ds(band - rim + first, count)], rim_buf.at[pl.ds(first, count)], rim_ss.at[at], rim_rs.at[at], t, lag_at(1))

    def rim_start(first, count, at):
        pl.when(l != lags - 1)(rim_copy(first, count, at).start)

    def rim_take(first, count, at):
        rows = pl.ds((band + rim - first - count) * shots, count * shots)

        @pl.when(is_first)
        def _():
            ht[rows, :] = jnp.zeros((count * shots, width), BF16)

        @pl.when(l != 0)
        def _():
            landed(rim_buf.at[pl.ds(first, count)], rim_rs.at[at])
            for q in range(first, first + count):
                ht[pl.ds((band + rim - 1 - q) * shots, shots), :] = rim_buf[q].T

    def slots(p):
        return pl.ds(pl.multiple_of(p * CAP, CAP), CAP)

    own_slots = pl.ds(pl.multiple_of(t * CAP, CAP), CAP)

    def src_copy(d):
        to = patch_at(d)
        return remote(src_out.at[slots(to)], src_in.at[own_slots], src_ss, src_rs, to, l)

    def src_start(d, carry):
        src_copy(d).start()
        return carry

    def rs_copy(s, d):
        to = lag_at(d)
        part = pl.ds(pl.multiple_of(to * chunk, chunk), chunk)
        return remote(sbuf.at[s, part], rbuf.at[s, l], rs_ss, rs_rs.at[s], t, to)

    def send_step(s):
        rows = pl.ds(s * shots, shots)
        shared = pl.ds(pl.multiple_of(given + width * (1 - core), width), given)
        acc[rows, shared] += got[rows, :]
        sbuf[s] = acc[rows, pl.ds(given, kept)].astype(BF16)
        for d in range(1, lags):
            rs_copy(s, d).start()

    own_shots = pl.ds(pl.multiple_of(l * chunk, chunk), chunk)

    last = steps - 1

    def lag_sum(s):
        total = acc[pl.ds(pl.multiple_of(s * shots + l * chunk, chunk), chunk), pl.ds(given, kept)]
        landed(rbuf.at[s, pl.ds(0, lags - 1)], rs_rs.at[s])
        for d in range(1, lags):
            total = total + rbuf[s, lag_at(d)].astype(F32)
        parts = [total[:, m * width : (m + 1) * width] for m in range(HALF + 1)]
        own = jnp.where(core == 0, parts[HALF], parts[0]) - source[pl.ds(s * chunk, chunk), :]
        return parts, own

    def owner(f):
        return patch_at(f - HALF + (HALF + 1) * core)

    def piece_rows(side, lag):
        return pl.ds(pl.multiple_of(side * shots + lag * chunk, chunk), chunk)

    def piece_copy(s, f):
        return remote(psend.at[s, f + core], pbuf.at[s, piece_rows(HALF - core, l)], p_ss, p_rs.at[s], owner(f), 0)

    def own_piece_copy(s):
        return remote(own_send.at[s], pbuf.at[s, piece_rows(0, l)], p_ss, p_rs.at[s], t, 0)

    def pieces(s):
        parts, own = lag_sum(s)
        for m in range(HALF + 1):
            psend[s, m] = parts[m].astype(BF16)
        for f in range(HALF):
            piece_copy(s, f).start()

        @pl.when(is_first)
        def _():
            pbuf[s, pl.ds(0, chunk), :] = own.astype(BF16)

        @pl.when(l != 0)
        def _():
            own_send[s] = own.astype(BF16)
            own_piece_copy(s).start()

    def piece_wait(s):
        landed(pbuf.at[s, pl.ds(chunk, (HALF + 1) * shots - chunk)], p_rs.at[s])

    def piece_sum(s, first, count):
        sides = [pbuf[s, pl.ds(side * shots + first, count), :].astype(F32) for side in range(HALF + 1)]
        return sides[0] + sides[1] + sides[2]

    def nb_copy(f):
        return remote(nsend.at[f + core], nbuf.at[1 - core], nb_ss, nb_rs, owner(f), l)

    def last_sum():
        parts, own = lag_sum(last)
        for m in range(HALF + 1):
            nsend[m] = parts[m]
        for f in range(HALF):
            nb_copy(f).start()
        return own

    def nb_sum(own):
        landed(nbuf, nb_rs)
        return own + nbuf[0] + nbuf[1]

    def density_of(right):
        return dot(right.astype(BF16), inv_ref[...]).astype(BF16)

    def ag_copy(s, d, sent):
        return remote(dens.at[s, own_shots], dens.at[s, own_shots], sent, ag_rs, t, lag_at(d))

    with jax.named_scope("first"):
        w_copy(0).wait()
        set_lag(0, 0, shots)
        lax.fori_loop(1, per, first_step, 0)
        for a in range(1, band // per):
            w_copy(a).wait()
            lax.fori_loop(a * per, (a + 1) * per, first_step, 0)
    with jax.named_scope("bar"):
        pl.semaphore_wait(barrier, jnp.where(is_first, lags - 1 + patches - 1 + 4 * (lags - 1), lags - 1 + patches - 1 + 4))
    with jax.named_scope("pair0"):
        pair_copy(0, 1, 0).start()
        rim_start(rim - 1, 1, 0)

    with jax.named_scope("prep"):
        recv = tile_ref.shape[1]
        diagonal = iota((recv, recv), 0) == iota((recv, recv), 1)

        def as_column(row):
            return jnp.sum(jnp.where(diagonal, row.astype(F32), 0.0), axis=1, keepdims=True)

        tile_col = as_column(tile_ref[...])
        panel_col = as_column(panel_ref[...])
        named = (tile_col == iota((recv, 128), 1).astype(F32)).astype(F32)
        earlier = (iota((recv, recv), 1) < iota((recv, recv), 0)).astype(BF16)
        rank = jnp.sum(dot(earlier, named.astype(BF16)) * named, axis=1, keepdims=True)
        slot = tile_col * CAP + rank
        placer = (slot == iota((recv, patches * CAP), 1).astype(F32)).astype(BF16)
        src_width = src_out.shape[1]
        mine = jnp.zeros((recv, src_width), F32)
        resid_copy.wait()
        for s in range(steps):
            lane, place = iota((shots, src_width), 0), iota((shots, src_width), 1)
            pick = (lane - l * chunk == place - s * chunk) & (place >= s * chunk) & (place < (s + 1) * chunk)
            mine = mine + dot(resid_ref[:, s, :], pick.astype(BF16))
        mine = jnp.where(iota((recv, src_width), 1) == steps * chunk, panel_col + 1.0, mine).astype(BF16)
        src_out[...] = dot_rows(placer, mine).astype(BF16)
        src_in[own_slots, :] = src_out[own_slots, :]

    with jax.named_scope("pairwait0"):
        pair_wait(0, 1)
    with jax.named_scope("send0"):
        send_step(0)
        lax.fori_loop(1, patches, src_start, 0)
        rim_start(0, rim - 1, 1)
    with jax.named_scope("later2"):
        set_lag(rim, shots, (steps - 1) * shots)
        lax.fori_loop(rim + 1, band, later_steps, 0)

    with jax.named_scope("rim1"):
        rim_take(rim - 1, 1, 0)
        lax.fori_loop(0, rim, second_step_rim, 0)
        pair_copy(1, 1, 1).start()

    with jax.named_scope("srcwait"):
        landed(src_in.at[pl.ds(0, (patches - 1) * CAP)], src_rs)
        inv_copy.wait()
    with jax.named_scope("src"):
        labels = src_in[:, pl.ds(steps * chunk, 1)].astype(F32)
        onto = (labels == (iota((patches * CAP, width), 1) + 1).astype(F32)).astype(BF16)
        source[...] = dot_rows(src_in[...], onto)

    with jax.named_scope("rs0"):
        pieces(0)
    with jax.named_scope("send1"):
        pair_wait(1, 1)
        send_step(1)
    with jax.named_scope("rim23"):
        rim_take(0, rim - 1, 1)
        lax.fori_loop(0, rim, last_steps_rim, 0)
        pair_copy(2, steps - 2, 2).start()
    with jax.named_scope("send2"):
        pair_wait(2, steps - 2)
        send_step(2)

    def place_of(i):
        return HALF * 2 if i == HALF else i - (i > HALF)

    def terms_rows(i, first, count):
        return pl.ds(i * shots + first, count)

    def ch_copy(n, i, g):
        return remote(csend.at[n - 1, terms_rows(i, g * group, group)], cgot.at[n - 1, g, place_of(i)], ch_ss, ch_rs.at[n - 1, g], patch_at(i - HALF), 0)

    def out_copy(i, lag):
        return remote(csend.at[last - 1, terms_rows(i, lag * chunk, chunk)], cbuf.at[place_of(i)], out_ss, out_rs, patch_at(i - HALF), lag)

    def spread_copy(s, part, lag):
        rows = pl.ds(part * chunk, chunk)
        return remote(dens.at[s, rows], dens.at[s, rows], sp_ss, ag_rs if part == 0 else sp_rs.at[s], t, lag)

    def others(d):
        return pl.when(lag_at(d) != 0)

    def new_terms(k, s, i, rows):
        return is_active(k, i) * dot(dens[s, rows, :], w_buf[k - 1, :, pl.ds(i * width, width)])

    def send_terms(n, g):
        rows = pl.ds(g * group, group)
        for i in (0, NEAR - 1, 1, NEAR - 2, *range(2, NEAR - 2)):
            value = new_terms(1, n - 1, i, rows)
            if n > 1:
                value = value + cacc[n - 2, i, rows, :]
            csend[n - 1, terms_rows(i, g * group, group), :] = value.astype(BF16)
            if n < last:
                if i != HALF:
                    ch_copy(n, i, g).start()
            else:
                for lag in range(g * group // chunk, (g + 1) * group // chunk):
                    if i == HALF and lag == 0:
                        cbuf[place_of(i)] = value[:chunk].astype(BF16)
                    else:
                        out_copy(i, lag).start()

    def older_terms(s):
        for n in range(s + 2, steps):
            for i in range(NEAR):
                value = new_terms(n - s, s, i, pl.ds(0, shots))
                if s > 0:
                    value = value + cacc[n - 2, i]
                cacc[n - 2, i] = value

    def finish(n, g):
        rest = -piece_sum(n, g * group, group) - csend[n - 1, terms_rows(HALF, g * group, group), :].astype(F32)
        landed(cgot.at[n - 1, g], ch_rs.at[n - 1, g])
        for i in range(NEAR - 1):
            rest = rest - cgot[n - 1, g, i].astype(F32)
        dens[n, pl.ds(g * group, group), :] = density_of(rest)

    def spread(s):
        for lag in range(1, lags):
            spread_copy(s, lag, lag).start()
            spread_copy(s, 0, lag).start()

    @pl.when(is_first)
    def _():
        with jax.named_scope("rs1"):
            pieces(1)
        with jax.named_scope("p0"):
            piece_wait(0)
        with jax.named_scope("terms1"):
            dens[0] = density_of(-piece_sum(0, 0, shots))
            for g in range(groups):
                send_terms(1, g)
            spread(0)
        with jax.named_scope("older1"):
            older_terms(0)
        with jax.named_scope("rs2"):
            pieces(2)
        with jax.named_scope("send3"):
            send_step(last)
        for n in range(1, last):
            with jax.named_scope(f"p{n}"):
                piece_wait(n)
            for g in range(groups):
                with jax.named_scope(f"finish{n}{g}"):
                    finish(n, g)
                with jax.named_scope(f"terms{n + 1}{g}"):
                    send_terms(n + 1, g)
                if n == last - 1 and g == 0:
                    with jax.named_scope("rs3"):
                        own_last[...] = last_sum()
            spread(n)
            if n == 1:
                with jax.named_scope("older2"):
                    older_terms(n)

    @pl.when(l != 0)
    def _():
        def pass_on(n):
            landed(dens.at[n, own_shots], sp_rs.at[n])
            for d in range(1, lags):
                others(d)(ag_copy(n, d, pass_ss).start)

        with jax.named_scope("rs1"):
            pieces(1)
        with jax.named_scope("rs2"):
            pieces(2)
        with jax.named_scope("send3"):
            send_step(last)
        with jax.named_scope("sp0"):
            pass_on(0)
        with jax.named_scope("rs3"):
            own_last[...] = last_sum()
        with jax.named_scope("sp"):
            for n in range(1, last):
                pass_on(n)

    with jax.named_scope("nblast"):
        rest = -nb_sum(own_last[...])
    with jax.named_scope("outwait"):
        @pl.when(is_first)
        def _():
            landed(cbuf.at[pl.ds(0, NEAR - 1)], out_rs)

        @pl.when(l != 0)
        def _():
            landed(cbuf, out_rs)

        for i in range(NEAR):
            rest = rest - cbuf[i].astype(F32)
    with jax.named_scope("dlast"):
        dens[last, own_shots, :] = density_of(rest)
        for d in range(1, lags):
            ag_copy(last, d, ag_ss).start()

    with jax.named_scope("aglast"):
        seven = pl.ds(0, (lags - 1) * chunk)

        @pl.when(is_first)
        def _():
            landed(dens.at[0, seven], ag_rs)

        @pl.when(l != 0)
        def _():
            landed(dens.at[:, seven], ag_rs)

    with jax.named_scope("fin"):
        for s in range(steps):
            out_ref[s] = dens[s].T
        landed(src_in.at[pl.ds(0, (patches - 1) * CAP)], src_ss)

        @pl.when(l != lags - 1)
        def _():
            landed(rim_buf.at[pl.ds(rim - 1, 1)], rim_ss.at[0])
            landed(rim_buf.at[pl.ds(0, rim - 1)], rim_ss.at[1])

        landed(rbuf.at[:, pl.ds(0, lags - 1)], rs_ss)
        landed(got, pair_ss)
        landed(nbuf, nb_ss)
        landed(dens.at[0, seven], ag_ss)

        @pl.when(is_first)
        def _():
            landed(pbuf.at[:, pl.ds(0, HALF * chunk)], p_ss)
            landed(cgot, ch_ss)
            landed(csend.at[last - 1, pl.ds(0, (NEAR * lags - 1) * chunk)], out_ss)
            landed(pbuf.at[:, pl.ds(0, 2 * (lags - 1) * chunk)], sp_ss)

        @pl.when(l != 0)
        def _():
            landed(pbuf.at[:, pl.ds(0, (HALF + 1) * chunk)], p_ss)
            landed(dens.at[pl.ds(0, last), pl.ds(0, (lags - 2) * chunk)], pass_ss)


def local(patches, lags, interaction, history, near_inverse, lag_ranges, receiver_tile, receiver_panel, residuals):
    band, width, cols = interaction.shape
    shots = history.shape[2]
    recv, steps, _ = residuals.shape
    chunk = shots // lags
    src_width = -(-(steps * chunk + 1) // 128) * 128
    per = 3 if band % 3 == 0 else 1
    any_space = pl.BlockSpec(memory_space=pl.ANY)
    vmem = pl.BlockSpec(memory_space=pltpu.VMEM)
    dma = pltpu.SemaphoreType.DMA
    out = pl.pallas_call(
        functools.partial(kernel, patches, lags),
        out_shape=jax.ShapeDtypeStruct((steps, width, shots), BF16),
        in_specs=[any_space, any_space, any_space, pl.BlockSpec(memory_space=pltpu.SMEM), vmem, vmem, any_space],
        out_specs=vmem,
        scratch_shapes=[
            pltpu.VMEM((band, width, cols), BF16),
            pltpu.VMEM((band, width, shots), BF16),
            pltpu.VMEM(near_inverse.shape, BF16),
            pltpu.VMEM((recv, steps, shots), BF16),
            pltpu.VMEM((steps - 1, width, shots), BF16),
            pltpu.VMEM(((band + steps - 1) * shots, width), BF16),
            pltpu.VMEM((steps * shots, cols), F32),
            pltpu.VMEM((steps * shots, HALF * width), F32),
            pltpu.VMEM((steps, shots, (HALF + 1) * width), BF16),
            pltpu.VMEM((steps, lags, chunk, (HALF + 1) * width), BF16),
            pltpu.VMEM((steps - 1, HALF + 1, chunk, width), BF16),
            pltpu.VMEM((steps - 1, chunk, width), BF16),
            pltpu.VMEM((steps - 1, (HALF + 1) * shots, width), BF16),
            pltpu.VMEM((HALF + 1, chunk, width), F32),
            pltpu.VMEM((2, chunk, width), F32),
            pltpu.VMEM((chunk, width), F32),
            pltpu.VMEM((patches * CAP, src_width), BF16),
            pltpu.VMEM((patches * CAP, src_width), BF16),
            pltpu.VMEM((src_width, width), F32),
            pltpu.VMEM((steps, shots, width), BF16),
            pltpu.VMEM((steps - 2, NEAR, shots, width), F32),
            pltpu.VMEM((steps - 1, NEAR * shots, width), BF16),
            pltpu.VMEM((steps - 2, GROUPS, NEAR - 1, shots // GROUPS, width), BF16),
            pltpu.VMEM((NEAR, chunk, width), BF16),
            dma((band // per,)), dma, dma, dma, dma((2,)), dma((2,)), dma, dma, dma, dma((steps,)), dma, dma((steps - 1,)), dma, dma,
            dma, dma, dma, dma, dma((3,)), dma, dma((steps - 2, GROUPS)), dma, dma, dma, dma((steps - 1,)),
        ],
        compiler_params=pltpu.CompilerParams(collective_id=0, has_side_effects=True, vmem_limit_bytes=60 * 1024 * 1024),
        name="march",
    )(
        interaction, history, near_inverse, lag_ranges, receiver_tile.reshape(1, recv), receiver_panel.reshape(1, recv),
        residuals,
    )
    return out


def solution(mesh):
    in_specs = (
        P("lag", "patch", None),
        P("lag", "patch", None),
        P("patch", None),
        P("patch", None),
        P("patch", None),
        P("patch"),
        P("patch", None, None),
    )
    body = functools.partial(local, mesh.shape["patch"], mesh.shape["lag"])
    return jax.shard_map(body, mesh=mesh, in_specs=in_specs, out_specs=P(None, "patch", None), check_vma=False)
```
